16 devices in a mesh: tp: 2 (over z), dp: 8 (over y, x, core).
Axes of the slice: x: 2, y: 2, z: 2, core: 2. Of those that a mesh axis runs over, the one named last changes fastest.
Arguments:
- hidden: bfloat16 [24, 384, 1024], P('dp')
- labels: int32 [24, 384], P('dp')
- loss_mask: int32 [24, 384], P('dp')
- ln_gain: float32 [1024], replicated
- ln_bias: float32 [1024], replicated
- w_query: bfloat16 [1024, 16, 64], P(None, 'tp')
- w_key: bfloat16 [1024, 16, 64], P(None, 'tp')
- w_value: bfloat16 [1024, 16, 64], P(None, 'tp')
- w_attn_out: bfloat16 [16, 64, 1024], P('tp')
- w_fc_in: bfloat16 [1024, 4096], P(None, 'tp')
- b_fc_in: float32 [4096], P('tp')
- w_fc_out: bfloat16 [4096, 1024], P('tp')
- b_fc_out: float32 [1024], replicated
- lnf_gain: float32 [1024], replicated
- lnf_bias: float32 [1024], replicated
- w_head: bfloat16 [1024, 50304], P(None, 'tp')
- b_head: float32 [50304], P('tp')
Outputs:
- output 1: float32 [], replicated
- output 2: bfloat16 [24, 384, 1024], P('dp')
- output 3: float32 [1024], replicated
- output 4: float32 [1024], replicated
- output 5: float32 [1024, 16, 64], P(None, 'tp')
- output 6: float32 [1024, 16, 64], P(None, 'tp')
- output 7: float32 [1024, 16, 64], P(None, 'tp')
- output 8: float32 [16, 64, 1024], P('tp')
- output 9: float32 [1024, 4096], P(None, 'tp')
- output 10: float32 [4096], P('tp')
- output 11: float32 [4096, 1024], P('tp')
- output 12: float32 [1024], replicated
- output 13: float32 [1024], replicated
- output 14: float32 [1024], replicated
- output 15: float32 [1024, 50304], P(None, 'tp')
- output 16: float32 [50304], P('tp')
All inputs are finite; a program needn't handle non-finite values.
Results may differ from the reference program's by a relative error of at most 0.0134912.
Values sent between devices are 32-bit elements.
A program may use at most 1 GiB of HBM per device.

```python
import jax
import jax.numpy as jnp
from jax import lax

BATCH_ROWS = 24
SEQ_LEN = 384
D_MODEL = 1024
N_HEADS = 16
HEAD_DIM = 64
FF_DIM = 4096
VOCAB_SIZE = 50304
ROT_DIM = HEAD_DIM // 4
LN_EPS = 1e-5
ROPE_BASE = 10000.0


def setup_inputs(seed: int = 0) -> dict:
    keys = jax.random.split(jax.random.key(seed), 17)

    def normal(index, shape, scale):
        return jax.random.normal(keys[index], shape, jnp.float32) * scale

    row_ids = jnp.arange(BATCH_ROWS)
    lengths = jax.random.randint(keys[1], (BATCH_ROWS,), SEQ_LEN // 8, SEQ_LEN + 1)
    lengths = jnp.where(row_ids == 0, SEQ_LEN, lengths)
    lengths = jnp.where(row_ids == BATCH_ROWS - 1, SEQ_LEN // 8, lengths)
    loss_mask = (jnp.arange(SEQ_LEN)[None, :] < lengths[:, None]).astype(jnp.int32)
    labels = jax.random.randint(keys[2], (BATCH_ROWS, SEQ_LEN), 0, VOCAB_SIZE)
    labels = labels.at[0, 0].set(0).at[0, 1].set(VOCAB_SIZE - 1)
    d_scale = D_MODEL ** -0.5
    return {
        'hidden': normal(0, (BATCH_ROWS, SEQ_LEN, D_MODEL), 1.0).astype(jnp.bfloat16),
        'labels': labels,
        'loss_mask': loss_mask,
        'ln_gain': 1.0 + normal(3, (D_MODEL,), 0.3),
        'ln_bias': normal(4, (D_MODEL,), 0.3),
        'w_query': normal(5, (D_MODEL, N_HEADS, HEAD_DIM), d_scale).astype(jnp.bfloat16),
        'w_key': normal(6, (D_MODEL, N_HEADS, HEAD_DIM), d_scale).astype(jnp.bfloat16),
        'w_value': normal(7, (D_MODEL, N_HEADS, HEAD_DIM), d_scale).astype(jnp.bfloat16),
        'w_attn_out': normal(8, (N_HEADS, HEAD_DIM, D_MODEL), d_scale).astype(jnp.bfloat16),
        'w_fc_in': normal(9, (D_MODEL, FF_DIM), d_scale).astype(jnp.bfloat16),
        'b_fc_in': normal(10, (FF_DIM,), 0.5),
        'w_fc_out': normal(11, (FF_DIM, D_MODEL), FF_DIM ** -0.5).astype(jnp.bfloat16),
        'b_fc_out': normal(12, (D_MODEL,), 0.5),
        'lnf_gain': 1.0 + normal(13, (D_MODEL,), 0.3),
        'lnf_bias': normal(14, (D_MODEL,), 0.3),
        'w_head': normal(15, (D_MODEL, VOCAB_SIZE), d_scale).astype(jnp.bfloat16),
        'b_head': normal(16, (VOCAB_SIZE,), 1.0) + jnp.linspace(-3.0, 3.0, VOCAB_SIZE),
    }


def bf16_grid(values):
    return values.astype(jnp.bfloat16).astype(jnp.float32)


def layer_norm(values, gain_vec, shift_vec):
    row_mean = jnp.mean(values, axis=-1, keepdims=True)
    centered = values - row_mean
    variance = jnp.mean(centered * centered, axis=-1, keepdims=True)
    return centered * lax.rsqrt(variance + LN_EPS) * gain_vec + shift_vec


def rope_tables(seq_count, rot_dim):
    half_rot = rot_dim // 2
    inv_freq = ROPE_BASE ** (-2.0 * jnp.arange(half_rot, dtype=jnp.float32) / rot_dim)
    angles = jnp.arange(seq_count, dtype=jnp.float32)[:, None] * inv_freq[None, :]
    return jnp.cos(angles)[:, None, :], jnp.sin(angles)[:, None, :]


def apply_rotary(tensor, cosine, sine_tab):
    rot_dim = 2 * cosine.shape[-1]
    pairs = tensor[..., :rot_dim].reshape(tensor.shape[:-1] + (rot_dim // 2, 2))
    even_part = pairs[..., 0]
    odd_part = pairs[..., 1]
    rotated = jnp.stack([even_part * cosine - odd_part * sine_tab, odd_part * cosine + even_part * sine_tab], axis=-1)
    return jnp.concatenate([rotated.reshape(tensor.shape[:-1] + (rot_dim,)), tensor[..., rot_dim:]], axis=-1)


def row_loss(params, hidden_row, label_row, mask_row, inv_count):
    (ln_gain, ln_bias, w_query, w_key, w_value, w_attn_out, w_fc_in, b_fc_in,
     w_fc_out, b_fc_out, lnf_gain, lnf_bias, w_head, b_head) = params
    seq_count = hidden_row.shape[0]
    cosine, sine_tab = rope_tables(seq_count, ROT_DIM)
    normed = bf16_grid(layer_norm(hidden_row, ln_gain, ln_bias))
    q_rot = bf16_grid(apply_rotary(jnp.einsum('td,dhe->the', normed, w_query), cosine, sine_tab))
    k_rot = bf16_grid(apply_rotary(jnp.einsum('td,dhe->the', normed, w_key), cosine, sine_tab))
    v_proj = bf16_grid(jnp.einsum('td,dhe->the', normed, w_value))
    causal = jnp.arange(seq_count)[None, :] <= jnp.arange(seq_count)[:, None]
    scores = jnp.einsum('qhe,khe->hqk', q_rot, k_rot) * (HEAD_DIM ** -0.5)
    probs = bf16_grid(jax.nn.softmax(jnp.where(causal[None], scores, -1e30), axis=-1))
    context = bf16_grid(jnp.einsum('hqk,khe->qhe', probs, v_proj))
    attn_out = jnp.einsum('qhe,hed->qd', context, w_attn_out)
    gelu_out = bf16_grid(jax.nn.gelu(jnp.dot(normed, w_fc_in) + b_fc_in, approximate=True))
    resid_out = hidden_row + attn_out + jnp.dot(gelu_out, w_fc_out) + b_fc_out
    final_norm = bf16_grid(layer_norm(resid_out, lnf_gain, lnf_bias))
    logits = jnp.dot(final_norm, w_head) + b_head
    log_norm = jax.nn.logsumexp(logits, axis=-1)
    target_logit = jnp.take_along_axis(logits, label_row[:, None], axis=-1)[:, 0]
    return jnp.sum(mask_row.astype(jnp.float32) * (log_norm - target_logit)) * inv_count


def reference(hidden, labels, loss_mask, ln_gain, ln_bias, w_query, w_key, w_value, w_attn_out,
              w_fc_in, b_fc_in, w_fc_out, b_fc_out, lnf_gain, lnf_bias, w_head, b_head):
    params = tuple(leaf.astype(jnp.float32) for leaf in (
        ln_gain, ln_bias, w_query, w_key, w_value, w_attn_out, w_fc_in, b_fc_in,
        w_fc_out, b_fc_out, lnf_gain, lnf_bias, w_head, b_head))
    inv_count = 1.0 / jnp.sum(loss_mask.astype(jnp.float32))
    checked = jax.checkpoint(row_loss)

    def total_loss(param_tuple, hidden_f32):
        per_row = lax.map(
            lambda row_args: checked(param_tuple, row_args[0], row_args[1], row_args[2], inv_count),
            (hidden_f32, labels, loss_mask))
        return jnp.sum(per_row)

    loss, vjp_fn = jax.vjp(total_loss, params, hidden.astype(jnp.float32))
    grads, grad_hidden = vjp_fn(jnp.ones_like(loss))
    (g_ln_gain, g_ln_bias, g_w_query, g_w_key, g_w_value, g_w_attn_out, g_w_fc_in, g_b_fc_in,
     g_w_fc_out, g_b_fc_out, g_lnf_gain, g_lnf_bias, g_w_head, g_b_head) = grads
    return (loss, grad_hidden.astype(jnp.bfloat16), g_ln_gain, g_ln_bias, g_w_query, g_w_key, g_w_value,
            g_w_attn_out, g_w_fc_in, g_b_fc_in, g_w_fc_out, g_b_fc_out, g_lnf_gain, g_lnf_bias,
            g_w_head, g_b_head)
```

```python
import functools
import jax
import jax.numpy as jnp
from jax import lax
from jax.experimental import pallas as pl
from jax.experimental.pallas import tpu as pltpu
from jax.sharding import PartitionSpec as P

LN_EPS = 1e-5
ROPE_BASE = 10000.0
DATA_SPECS = (P('dp', None, None), P('dp', None), P('dp', None))
PARAM_SPECS = (P(None), P(None), P(None, 'tp', None), P(None, 'tp', None), P(None, 'tp', None),
               P('tp', None, None), P(None, 'tp'), P('tp'), P('tp', None), P(None), P(None), P(None),
               P(None, 'tp'), P('tp'))


def norm_stats(values):
    row_mean = jnp.mean(values, axis=-1, keepdims=True)
    centered = values - row_mean
    inv_std = lax.rsqrt(jnp.mean(centered * centered, axis=-1, keepdims=True) + LN_EPS)
    return centered * inv_std, inv_std


def norm_backward(grad_out, x_hat, inv_std, gain_vec):
    grad_hat = grad_out * gain_vec
    mean_grad = jnp.mean(grad_hat, axis=-1, keepdims=True)
    mean_proj = jnp.mean(grad_hat * x_hat, axis=-1, keepdims=True)
    grad_in = inv_std * (grad_hat - mean_grad - x_hat * mean_proj)
    return grad_in, jnp.sum(grad_out * x_hat, axis=(0, 1)), jnp.sum(grad_out, axis=(0, 1))


def rope_tables(seq_count, rot_dim):
    half_rot = rot_dim // 2
    inv_freq = ROPE_BASE ** (-2.0 * jnp.arange(half_rot, dtype=jnp.float32) / rot_dim)
    angles = jnp.arange(seq_count, dtype=jnp.float32)[:, None] * inv_freq[None, :]
    return jnp.cos(angles)[:, None, :], jnp.sin(angles)[:, None, :]


def apply_rotary(tensor, cosine, sine_tab):
    rot_dim = 2 * cosine.shape[-1]
    pairs = tensor[..., :rot_dim].reshape(tensor.shape[:-1] + (rot_dim // 2, 2))
    even_part = pairs[..., 0]
    odd_part = pairs[..., 1]
    rotated = jnp.stack([even_part * cosine - odd_part * sine_tab, odd_part * cosine + even_part * sine_tab], axis=-1)
    return jnp.concatenate([rotated.reshape(tensor.shape[:-1] + (rot_dim,)), tensor[..., rot_dim:]], axis=-1)


TOK_TILE = 512
COL_BLK = 512
ELEM_ROWS = 64
PAD_ROWS = 1024
NEVER = 1e30
COST_SCALE = 13 * 10**9


def pack_kernel(starts, z_ref, aux_ref, z_out, aux_out):
    row = pl.program_id(0)
    span = z_ref.shape[0]
    at = pl.multiple_of(starts[row], 16)
    z_out[pl.ds(at, span), :] = z_ref[...].astype(jnp.bfloat16)
    aux_out[pl.ds(at, span), :] = aux_ref[...]

    @pl.when(row == pl.num_programs(0) - 1)
    def _():
        end = pl.multiple_of(starts[row + 1], 16)
        z_out[pl.ds(end, PAD_ROWS), :] = jnp.zeros((PAD_ROWS, z_out.shape[1]), jnp.bfloat16)
        aux_out[pl.ds(end, PAD_ROWS), :] = jnp.full((PAD_ROWS, 128), NEVER, jnp.float32)


def pack_tokens(starts, z_all, aux_all, n_rows):
    total, dim = z_all.shape
    span = total // n_rows
    return pl.pallas_call(
        pack_kernel,
        grid_spec=pltpu.PrefetchScalarGridSpec(
            num_scalar_prefetch=1, grid=(n_rows,),
            in_specs=[pl.BlockSpec((span, dim), lambda r, s: (r, 0)), pl.BlockSpec((span, 128), lambda r, s: (r, 0))],
            out_specs=[pl.BlockSpec((total + PAD_ROWS, dim), lambda r, s: (0, 0)),
                       pl.BlockSpec((total + PAD_ROWS, 128), lambda r, s: (0, 0))]),
        out_shape=[jax.ShapeDtypeStruct((total + PAD_ROWS, dim), jnp.bfloat16),
                   jax.ShapeDtypeStruct((total + PAD_ROWS, 128), jnp.float32)],
        compiler_params=pltpu.CompilerParams(vmem_limit_bytes=62 * 2**20, dimension_semantics=("arbitrary",)),
        cost_estimate=pl.CostEstimate(flops=10**10, bytes_accessed=6 * 10**7, transcendentals=0),
    )(starts, z_all, aux_all)


def head_kernel(where_ref, z_ref, aux_ref, w_ref, b_ref, *rest):
    grad_own, grad_full, bias_own, logit_buf, prob_buf, bias_buf = rest[-6:]
    n_tiles = where_ref[0]
    first = (where_ref[1] + pl.program_id(0)) * COL_BLK
    grad_own[...] = jnp.zeros_like(grad_own)
    bias_own[...] = jnp.zeros_like(bias_own)
    bias_buf[...] = jnp.broadcast_to(b_ref[...], (128, COL_BLK)).T
    groups = TOK_TILE // 128

    def tile(t):
        return pl.ds(pl.multiple_of(t * TOK_TILE, TOK_TILE), TOK_TILE)

    def logits(t, slot):
        logit_buf[slot] = lax.dot_general(w_ref[...], z_ref[tile(t), :], (((1,), (1,)), ((), ())),
                                          preferred_element_type=jnp.float32)

    def probs(t, slot):
        lse = aux_ref[0:1, tile(t)]
        label = aux_ref[1:2, tile(t)] - first.astype(jnp.float32)
        weight = aux_ref[2:3, tile(t)]
        for c in range(0, COL_BLK, ELEM_ROWS):
            rows = slice(c, c + ELEM_ROWS)
            bias = jnp.concatenate([bias_buf[rows, :]] * groups, axis=1)
            ids = (lax.broadcasted_iota(jnp.int32, (ELEM_ROWS, 1), 0) + c).astype(jnp.float32)
            g = jnp.exp((logit_buf[slot, rows, :] + bias) - lse) - jnp.where(ids == label, weight, 0.0)
            part = g[:, :128]
            for k in range(1, groups):
                part = part + g[:, k * 128:(k + 1) * 128]
            bias_own[rows, :] += part
            prob_buf[slot, rows, :] = g.astype(jnp.bfloat16)

    def weights(t, slot):
        grad_own[...] += jnp.dot(prob_buf[slot], z_ref[tile(t), :], preferred_element_type=jnp.float32)

    logits(0, 0)

    def pair(u, carry):
        t = 2 * u
        logits(t + 1, 1)
        probs(t, 0)
        weights(t, 0)
        logits(t + 2, 0)
        probs(t + 1, 1)
        weights(t + 1, 1)
        return carry

    lax.fori_loop(0, n_tiles // 2, pair, 0)

    @pl.when(n_tiles % 2 == 1)
    def _():
        probs(n_tiles - 1, 0)
        weights(n_tiles - 1, 0)

    grad_full[...] = grad_own[...]


def head_chunk(n_blk, where, z_pack, aux_pack, w_head, b_head, grad_full):
    rows, dim = z_pack.shape
    vocab = w_head.shape[0]
    once = pl.Buffered(buffer_count=1)
    in_specs = [pl.BlockSpec((rows, dim), lambda j, s: (0, 0), pipeline_mode=once),
                pl.BlockSpec((8, rows), lambda j, s: (0, 0), pipeline_mode=once),
                pl.BlockSpec((COL_BLK, dim), lambda j, s: (s[1] + j, 0)),
                pl.BlockSpec((1, COL_BLK), lambda j, s: (0, s[1] + j))]
    operands = [where, z_pack, aux_pack, w_head, b_head]
    aliases = {}
    if grad_full is not None:
        in_specs.append(pl.BlockSpec(memory_space=pl.ANY))
        operands.append(grad_full)
        aliases = {5: 1}
    return pl.pallas_call(
        head_kernel,
        grid_spec=pltpu.PrefetchScalarGridSpec(
            num_scalar_prefetch=1, grid=(n_blk,), in_specs=in_specs,
            out_specs=[pl.BlockSpec((COL_BLK, dim), lambda j, s: (j, 0)),
                       pl.BlockSpec((COL_BLK, dim), lambda j, s: (s[1] + j, 0)),
                       pl.BlockSpec((COL_BLK, 128), lambda j, s: (j, 0))],
            scratch_shapes=[pltpu.VMEM((2, COL_BLK, TOK_TILE), jnp.float32),
                            pltpu.VMEM((2, COL_BLK, TOK_TILE), jnp.bfloat16),
                            pltpu.VMEM((COL_BLK, 128), jnp.float32)]),
        out_shape=[jax.ShapeDtypeStruct((n_blk * COL_BLK, dim), jnp.float32),
                   jax.ShapeDtypeStruct((vocab, dim), jnp.float32),
                   jax.ShapeDtypeStruct((n_blk * COL_BLK, 128), jnp.float32)],
        input_output_aliases=aliases,
        compiler_params=pltpu.CompilerParams(vmem_limit_bytes=50 * 2**20, dimension_semantics=("arbitrary",)),
        cost_estimate=pl.CostEstimate(flops=COST_SCALE * n_blk, bytes_accessed=6 * 10**7, transcendentals=0),
    )(*operands)


def place_kernel(where_ref, src_ref, full_ref, out_ref):
    out_ref[...] = src_ref[...]


def place_chunk(where, received, grad_full):
    width, dim = received.shape
    return pl.pallas_call(
        place_kernel,
        grid_spec=pltpu.PrefetchScalarGridSpec(
            num_scalar_prefetch=1, grid=(width // COL_BLK,),
            in_specs=[pl.BlockSpec((COL_BLK, dim), lambda j, s: (j, 0)), pl.BlockSpec(memory_space=pl.ANY)],
            out_specs=pl.BlockSpec((COL_BLK, dim), lambda j, s: (s[0] + j, 0))),
        out_shape=jax.ShapeDtypeStruct(grad_full.shape, jnp.float32),
        input_output_aliases={2: 0},
        compiler_params=pltpu.CompilerParams(vmem_limit_bytes=32 * 2**20, dimension_semantics=("arbitrary",)),
        cost_estimate=pl.CostEstimate(flops=10**8, bytes_accessed=8 * dim * width, transcendentals=0),
    )(where, received, grad_full)


class HeadGradients:
    def __init__(self, z_all, aux_all, lengths, w_head, b_head):
        self.w_rows, self.vocab = w_head.T, w_head.shape[1]
        self.half = -(-self.vocab // (2 * COL_BLK))
        self.bias_row = jnp.pad(b_head, (0, 2 * self.half * COL_BLK - self.vocab))[None, :]
        padded = (lengths + 15) // 16 * 16
        ends = jnp.cumsum(padded)
        starts = jnp.concatenate([jnp.zeros((1,), jnp.int32), ends])
        self.z_pack, aux_pack = pack_tokens(starts, z_all, aux_all, lengths.shape[0])
        self.aux_pack = aux_pack[:, :8].T
        self.n_tiles = (ends[-1] + TOK_TILE - 1) // TOK_TILE
        self.core = lax.axis_index('dp') % 2
        self.swap = [(i, i ^ 1) for i in range(lax.axis_size('dp'))]
        self.full, self.waiting, self.bias_parts, self.at = None, [], [], 0

    def after(self, values):
        self.n_tiles, *values = lax.optimization_barrier((self.n_tiles, *values))
        return values

    def chunk(self, size):
        where = jnp.stack([self.n_tiles, self.core * self.half + self.at])
        own, self.full, bias_part = head_chunk(size, where, self.z_pack, self.aux_pack, self.w_rows,
                                               self.bias_row, self.full)
        self.bias_parts.append(jnp.sum(bias_part, axis=1))
        self.waiting.append((self.at, lax.ppermute(own, 'dp', self.swap)))
        self.at += size

    def place(self):
        first, received = self.waiting.pop(0)
        self.full = place_chunk(jnp.stack([(1 - self.core) * self.half + first]), received, self.full)

    def result(self):
        own = jnp.concatenate(self.bias_parts)
        other = lax.ppermute(own, 'dp', self.swap)
        bias = jnp.where(self.core == 0, jnp.concatenate([own, other]), jnp.concatenate([other, own]))
        return self.full.T, bias[:self.vocab]


def solution(mesh):
    def local_step(hidden, labels, loss_mask, ln_gain, ln_bias, w_query, w_key, w_value, w_attn_out,
                   w_fc_in, b_fc_in, w_fc_out, b_fc_out, lnf_gain, lnf_bias, w_head, b_head):
        seq_count = hidden.shape[1]
        head_dim = w_query.shape[2]
        vocab_loc = w_head.shape[1]
        score_scale = head_dim ** -0.5
        cosine, sine_tab = rope_tables(seq_count, head_dim // 4)
        causal = jnp.arange(seq_count)[None, :] <= jnp.arange(seq_count)[:, None]
        resid_in = hidden.astype(jnp.float32)
        ln_hat, ln_inv = norm_stats(resid_in)
        normed = (ln_hat * ln_gain + ln_bias).astype(jnp.bfloat16)
        q_rot = apply_rotary(jnp.einsum('btd,dhe->bthe', normed, w_query, preferred_element_type=jnp.float32),
                             cosine, sine_tab).astype(jnp.bfloat16)
        k_rot = apply_rotary(jnp.einsum('btd,dhe->bthe', normed, w_key, preferred_element_type=jnp.float32),
                             cosine, sine_tab).astype(jnp.bfloat16)
        v_proj = jnp.einsum('btd,dhe->bthe', normed, w_value, preferred_element_type=jnp.float32).astype(jnp.bfloat16)
        scores = jnp.einsum('bqhe,bkhe->bhqk', q_rot, k_rot, preferred_element_type=jnp.float32) * score_scale
        probs = jax.nn.softmax(jnp.where(causal, scores, -1e30), axis=-1)
        probs_bf = probs.astype(jnp.bfloat16)
        context = jnp.einsum('bhqk,bkhe->bqhe', probs_bf, v_proj, preferred_element_type=jnp.float32).astype(jnp.bfloat16)
        pre_act = jnp.einsum('btd,df->btf', normed, w_fc_in, preferred_element_type=jnp.float32) + b_fc_in
        gelu_out, gelu_vjp = jax.vjp(functools.partial(jax.nn.gelu, approximate=True), pre_act)
        gelu_bf = gelu_out.astype(jnp.bfloat16)
        block_part = (jnp.einsum('crif,ife->cre', context, w_attn_out, preferred_element_type=jnp.float32)
                      + jnp.einsum('btf,fd->btd', gelu_bf, w_fc_out, preferred_element_type=jnp.float32))
        mask_f = loss_mask.astype(jnp.float32)
        token_count = lax.psum(jnp.sum(mask_f), 'dp')
        block_sum, token_count = lax.optimization_barrier((lax.psum(block_part, 'tp'), token_count))
        resid_out = resid_in + block_sum + b_fc_out
        fin_hat, fin_inv = norm_stats(resid_out)
        final_f32 = fin_hat * lnf_gain + lnf_bias
        final_bf = final_f32.astype(jnp.bfloat16)
        z_all = lax.all_gather(final_f32.reshape(-1, final_f32.shape[-1]), 'dp', axis=0, tiled=True)
        logits = jnp.einsum('btd,dv->btv', final_bf, w_head, preferred_element_type=jnp.float32) + b_head
        part_max = jnp.max(logits, axis=-1)
        local_label = labels - lax.axis_index('tp') * vocab_loc
        is_target = jnp.arange(vocab_loc) == local_label[..., None]
        stats = lax.all_gather(jnp.stack([part_max, jnp.sum(jnp.exp(logits - part_max[..., None]), axis=-1),
                                          jnp.sum(jnp.where(is_target, logits, 0.0), axis=-1)]), 'tp')
        glob_max = jnp.max(stats[:, 0], axis=0)
        exp_sum = jnp.sum(stats[:, 1] * jnp.exp(stats[:, 0] - glob_max), axis=0)
        target_logit = jnp.sum(stats[:, 2], axis=0)
        log_norm = glob_max + jnp.log(exp_sum)
        tok_weight = mask_f / token_count
        loss_part = jnp.sum(tok_weight * (log_norm - target_logit))
        grad_logits = (jnp.exp(logits - log_norm[..., None]) - jnp.where(is_target, 1.0, 0.0)) * tok_weight[..., None]
        grad_logits_bf = grad_logits.astype(jnp.bfloat16)
        grad_final_part = jnp.einsum('btv,dv->btd', grad_logits_bf, w_head, preferred_element_type=jnp.float32)
        active = mask_f > 0.0
        aux_loc = jnp.stack([jnp.where(active, log_norm + jnp.log(token_count), NEVER),
                             jnp.where(active, local_label.astype(jnp.float32), -1.0), tok_weight])
        grad_final_part, aux_loc = lax.optimization_barrier((grad_final_part, aux_loc))
        aux_all = lax.all_gather(aux_loc, 'dp', axis=1, tiled=True)
        lengths = jnp.sum((aux_all[2] > 0.0).astype(jnp.int32), axis=-1)
        aux_all = jnp.pad(aux_all.reshape(3, -1).T, ((0, 0), (0, 125)))
        head = HeadGradients(z_all, aux_all, lengths, w_head, b_head)
        grad_final = lax.psum(grad_final_part, 'tp')
        head.chunk(max(1, head.half * 4 // 25))
        grad_final, head.bias_parts[0] = lax.optimization_barrier((grad_final, head.bias_parts[0]))
        grad_resid, grad_lnf_gain, grad_lnf_bias = norm_backward(grad_final, fin_hat, fin_inv, lnf_gain)
        grad_b_fc_out = jnp.sum(grad_resid, axis=(0, 1))
        grad_block = grad_resid.astype(jnp.bfloat16)
        grad_w_fc_out = jnp.einsum('btf,btd->fd', gelu_bf, grad_block, preferred_element_type=jnp.float32)
        grad_w_attn_out = jnp.einsum('crif,cre->ife', context, grad_block, preferred_element_type=jnp.float32)
        grad_w_fc_out, grad_w_attn_out, grad_block = lax.optimization_barrier((grad_w_fc_out, grad_w_attn_out, grad_block))
        early = lax.psum((grad_w_fc_out, grad_w_attn_out), 'dp')
        grad_gelu = jnp.einsum('btd,fd->btf', grad_block, w_fc_out, preferred_element_type=jnp.float32)
        grad_pre = gelu_vjp(grad_gelu)[0]
        grad_b_fc_in = jnp.sum(grad_pre, axis=(0, 1))
        grad_pre_bf = grad_pre.astype(jnp.bfloat16)
        grad_w_fc_in = jnp.einsum('btd,btf->df', normed, grad_pre_bf, preferred_element_type=jnp.float32)
        grad_context = jnp.einsum('cre,ife->crif', grad_block, w_attn_out, preferred_element_type=jnp.float32).astype(jnp.bfloat16)
        grad_v = jnp.einsum('bhqk,bqhe->bkhe', probs_bf, grad_context, preferred_element_type=jnp.float32).astype(jnp.bfloat16)
        grad_probs = jnp.einsum('bqhe,bkhe->bhqk', grad_context, v_proj, preferred_element_type=jnp.float32)
        grad_scores = (probs * (grad_probs - jnp.sum(grad_probs * probs, axis=-1, keepdims=True)) * score_scale).astype(jnp.bfloat16)
        grad_q = apply_rotary(jnp.einsum('bhqk,bkhe->bqhe', grad_scores, k_rot, preferred_element_type=jnp.float32),
                              cosine, -sine_tab).astype(jnp.bfloat16)
        grad_k = apply_rotary(jnp.einsum('bhqk,bqhe->bkhe', grad_scores, q_rot, preferred_element_type=jnp.float32),
                              cosine, -sine_tab).astype(jnp.bfloat16)
        grad_w_query = jnp.einsum('btd,bthe->dhe', normed, grad_q, preferred_element_type=jnp.float32)
        grad_w_key = jnp.einsum('btd,bthe->dhe', normed, grad_k, preferred_element_type=jnp.float32)
        grad_w_value = jnp.einsum('btd,bthe->dhe', normed, grad_v, preferred_element_type=jnp.float32)
        grad_normed_part = (jnp.einsum('bthe,dhe->btd', grad_q, w_query, preferred_element_type=jnp.float32)
                            + jnp.einsum('bthe,dhe->btd', grad_k, w_key, preferred_element_type=jnp.float32)
                            + jnp.einsum('bthe,dhe->btd', grad_v, w_value, preferred_element_type=jnp.float32)
                            + jnp.einsum('btf,df->btd', grad_pre_bf, w_fc_in, preferred_element_type=jnp.float32))
        grad_normed_part, *late = head.after((grad_normed_part, grad_w_query, grad_w_key, grad_w_value, grad_w_fc_in))
        grad_normed = lax.psum(grad_normed_part, 'tp')
        left = head.half - head.at
        head.chunk(left * 10 // 21)
        head.chunk(left * 8 // 21)
        head.place()
        head.chunk(head.half - head.at)
        while head.waiting:
            head.place()
        grad_w_head, grad_b_head = head.result()
        grad_ln_in, grad_ln_gain, grad_ln_bias = norm_backward(grad_normed, ln_hat, ln_inv, ln_gain)
        grad_hidden = (grad_resid + grad_ln_in).astype(jnp.bfloat16)
        g_fc_out, g_attn_out, *late = lax.optimization_barrier((*early, *late))
        g_query, g_key, g_value, g_fc_in = lax.psum(tuple(late), 'dp')
        small = (loss_part[None], grad_ln_gain, grad_ln_bias, grad_b_fc_in, grad_b_fc_out, grad_lnf_gain, grad_lnf_bias)
        flat = jnp.concatenate(small)
        tiles = -(-flat.shape[0] // 1024) * 8
        flat = jnp.pad(flat, (0, tiles * 128 - flat.shape[0])).reshape(tiles, 128)
        small_sum = jnp.sum(lax.all_gather(flat, 'dp', axis=0, tiled=True).reshape(-1, tiles, 128), axis=0).reshape(-1)
        cuts = [small[0].shape[0]]
        for part in small[1:-1]:
            cuts.append(cuts[-1] + part.shape[0])
        loss, g_ln_gain, g_ln_bias, g_b_in, g_b_out, g_lnf_gain, g_lnf_bias = jnp.split(
            small_sum[:sum(part.shape[0] for part in small)], cuts)
        loss = loss[0]
        return (loss, grad_hidden, g_ln_gain, g_ln_bias, g_query, g_key, g_value, g_attn_out, g_fc_in, g_b_in,
                g_fc_out, g_b_out, g_lnf_gain, g_lnf_bias, grad_w_head, grad_b_head)

    return jax.shard_map(local_step, mesh=mesh, in_specs=DATA_SPECS + PARAM_SPECS,
                         out_specs=(P(), P('dp', None, None)) + PARAM_SPECS, check_vma=False)
```
